32 devices in a mesh: mem: 2 (over y), lat: 4 (over z), lon: 4 (over x, core).
Axes of the slice: x: 2, y: 2, z: 4, core: 2. Of those that a mesh axis runs over, the one named last changes fastest.
Arguments:
- control: bfloat16 [62, 3, 4, 4, 73728], P('mem', None, 'lat', 'lon'), may hold values from -6 to 6
- perturbs: bfloat16 [62, 3, 4, 4, 73728], P('mem', None, 'lat', 'lon'), may hold values from -0.75 to 0.75
- static_input: bfloat16 [3, 4, 4, 73728], P(None, 'lat', 'lon'), may hold values from -6 to 6
- lat_basis: bfloat16 [768, 384], replicated, may hold values from -0.21875 to 0.21875
- local_spectrum: float32 [384, 768], P(None, 'lat'), may hold values from 0.1 to 1
- static_spectrum: float32 [384, 768], P(None, 'lat'), may hold values from 0.1 to 1
- static_weight: float32 [3], replicated, may hold values from 0.2 to 0.8
Outputs:
- increment: float32 [3, 4, 4, 73728], P(None, 'lat', 'lon')
The draws below stay inside these ranges and needn't reach their ends.
All inputs are finite; a program needn't handle non-finite values.
Results may differ from the reference program's by a relative error of at most 0.0073.
Values may be sent and summed in bfloat16 or wider, within the bound.
No kernel may reach another device: no remote copies, remote signals or barrier semaphores. Data moves between devices by JAX's collectives and lax.ppermute only.
A program may use at most 128 MiB of HBM per device.

```python
import math
import jax
import jax.numpy as jnp
from jax import lax

NLON = 1536
NLAT = 768
KLON = 768
KLAT = 384
LEV = 3
MEMBERS = 62
CELLS = 73728
N_LAT = 4
N_LON = 4


def block_levels(own_key, shape, cuts, low, high):
    factor_of, own = 1.0, jax.random.fold_in(own_key, 6)
    for axis_at, parts in cuts:
        heights = jnp.exp(jax.random.uniform(jax.random.fold_in(own, axis_at), (parts,), jnp.float32, low / len(cuts), high / len(cuts)))
        factor_of = factor_of * jnp.repeat(heights, shape[axis_at] // parts).reshape([-1 if axis == axis_at else 1 for axis in range(len(shape))])
    return factor_of


def gaussian(own_key, dims, scale, limit, shards=(), held_as=jnp.bfloat16):
    result = jax.random.normal(own_key, dims, jnp.float32) * scale
    if len(shards) > 0:
        result = block_levels(own_key, dims, shards, -0.22, 0.18) * result
    return jnp.clip(result, min=-limit, max=limit).astype(held_as)


def setup_inputs(seed: int = 0) -> dict:
    arg_keys = jax.random.split(jax.random.key(seed), 8)
    control = gaussian(arg_keys[0], (MEMBERS, LEV, N_LAT, N_LON, CELLS), 1.0, 6.0, ((0, 2), (2, 4), (3, 4)))
    perturbs = gaussian(arg_keys[1], (MEMBERS, LEV, N_LAT, N_LON, CELLS), 0.125, 0.75, ((0, 2), (2, 4), (3, 4)))
    static_input = gaussian(arg_keys[2], (LEV, N_LAT, N_LON, CELLS), 1.0, 6.0, ((1, 4), (2, 4)))
    lat_basis = gaussian(arg_keys[3], (NLAT, KLAT), NLAT ** -0.5, 0.21875)
    local_spectrum = jnp.clip(jnp.exp(math.log(1.0) - 2.3025851 * jax.random.uniform(arg_keys[4], (KLAT, KLON), jnp.float32) ** block_levels(arg_keys[4], (KLAT, KLON), ((1, 4),), -0.2, 0.2)), 0.1, 1.0)
    static_spectrum = jnp.clip(jnp.exp(math.log(1.0) - 2.3025851 * jax.random.uniform(arg_keys[5], (KLAT, KLON), jnp.float32) ** block_levels(arg_keys[5], (KLAT, KLON), ((1, 4),), -0.2, 0.2)), 0.1, 1.0)
    static_weight = jnp.clip(jax.random.uniform(arg_keys[6], (LEV,), jnp.float32, 0.2, 0.8), 0.2, 0.8)
    return dict(control=control, perturbs=perturbs, static_input=static_input, lat_basis=lat_basis, local_spectrum=local_spectrum, static_spectrum=static_spectrum, static_weight=static_weight)


def zonal_table():
    half = KLON // 2
    points = jnp.arange(NLON, dtype=jnp.int32)
    column = jnp.arange(KLON, dtype=jnp.int32)
    wave = jnp.where(column < half, column, column - half + 1)
    phase = points[:, None] * wave[None, :] % NLON
    angle = 2.0 * jnp.pi / NLON * phase.astype(jnp.float32)
    scale = jnp.sqrt(jnp.float32(2.0 / NLON))
    values = jnp.where(column[None, :] < half, jnp.cos(angle), jnp.sin(angle)) * scale
    return values.astype(jnp.bfloat16)

def to_plain(blocks):
    lead = blocks.shape[:-3]
    count = len(lead)
    lat_rows = NLAT // N_LAT
    lon_cols = NLON // N_LON
    shaped = blocks.reshape(lead + (N_LAT, N_LON, lat_rows, lon_cols))
    shaped = jnp.moveaxis(shaped, count + 2, count + 1)
    return shaped.reshape(lead + (NLAT, NLON))

def to_blocks(plain):
    lead = plain.shape[:-2]
    count = len(lead)
    lat_rows = NLAT // N_LAT
    lon_cols = NLON // N_LON
    shaped = plain.reshape(lead + (N_LAT, lat_rows, N_LON, lon_cols))
    shaped = jnp.moveaxis(shaped, count + 1, count + 2)
    return shaped.reshape(lead + (N_LAT, N_LON, lat_rows * lon_cols))

def filter_fields(fields, spectrum, zonal, merid):
    zonal_f = zonal.astype(jnp.float32)
    merid_f = merid.astype(jnp.float32)
    waves = jnp.einsum('lyn,nk->lyk', fields.astype(jnp.float32), zonal_f).astype(jnp.bfloat16)
    coef = jnp.einsum('lyk,yj->ljk', waves.astype(jnp.float32), merid_f) * spectrum[None]
    scaled = coef.astype(jnp.bfloat16)
    back = jnp.einsum('ljk,yj->lyk', scaled.astype(jnp.float32), merid_f).astype(jnp.bfloat16)
    grid = jnp.einsum('lyk,nk->lyn', back.astype(jnp.float32), zonal_f).astype(jnp.bfloat16)
    return grid

def reference(control, perturbs, static_input, lat_basis, local_spectrum, static_spectrum, static_weight):
    zonal = zonal_table()

    def add_member(total, pair):
        alpha, pert = pair
        grid = filter_fields(to_plain(alpha), local_spectrum, zonal, lat_basis)
        return (total + to_plain(pert).astype(jnp.float32) * grid.astype(jnp.float32), None)
    start = jnp.zeros((LEV, NLAT, NLON), jnp.float32)
    ensemble, unused = lax.scan(add_member, start, (control, perturbs))
    static_part = filter_fields(to_plain(static_input), static_spectrum, zonal, lat_basis).astype(jnp.float32)
    weight = static_weight[:, None, None]
    return to_blocks(weight * static_part + (1.0 - weight) * ensemble)
```

```python
import functools

import jax
import jax.numpy as jnp
from jax import lax
from jax.experimental import pallas as pl
from jax.experimental.pallas import tpu as pltpu
from jax.sharding import PartitionSpec as P

NLON = 1536
NLAT = 768
KLON = 768


def zonal_table():
    half = KLON // 2
    points = jnp.arange(NLON, dtype=jnp.int32)
    column = jnp.arange(KLON, dtype=jnp.int32)
    wave = jnp.where(column < half, column, column - half + 1)
    phase = points[:, None] * wave[None, :] % NLON
    angle = 2.0 * jnp.pi / NLON * phase.astype(jnp.float32)
    scale = jnp.sqrt(jnp.float32(2.0 / NLON))
    values = jnp.where(column[None, :] < half, jnp.cos(angle), jnp.sin(angle)) * scale
    return values.astype(jnp.bfloat16)


def shards_general(
    control, perturbs, static_input, lat_basis, local_spectrum, static_spectrum, static_weight
):
    mem_dev, levels = (control.shape[0], control.shape[1])
    cell_count = control.shape[-1]
    lat_rows = NLAT // lax.axis_size("lat")
    lon_cols = cell_count // lat_rows
    fields = jnp.concatenate([control, static_input[None]], 0).reshape(-1, lat_rows, lon_cols)
    per_lon = fields.shape[0] // lax.axis_size("lon")
    field_index = lax.axis_index("lon") * per_lon + jnp.arange(per_lon, dtype=jnp.int32)
    is_static = field_index >= mem_dev * levels
    first_mem = (lax.axis_index("mem") == 0).astype(jnp.float32)
    zonal = zonal_table()
    strips = lax.all_to_all(fields, "lon", split_axis=0, concat_axis=2, tiled=True)
    waves = jnp.einsum("bxn,nk->kbx", strips, zonal, preferred_element_type=jnp.float32).astype(
        jnp.bfloat16
    )
    merid = lax.all_to_all(waves, "lat", split_axis=0, concat_axis=2, tiled=True)
    coef = jnp.einsum("kby,yj->kbj", merid, lat_basis, preferred_element_type=jnp.float32)
    spectrum = jnp.where(
        is_static[None, :, None], static_spectrum.T[:, None, :], local_spectrum.T[:, None, :]
    )
    scaled = (coef * spectrum).astype(jnp.bfloat16)
    back = jnp.einsum("kbj,yj->kby", scaled, lat_basis, preferred_element_type=jnp.float32).astype(
        jnp.bfloat16
    )
    zonal_rows = lax.all_to_all(back, "lat", split_axis=2, concat_axis=0, tiled=True)
    grid = jnp.einsum("kbx,nk->bxn", zonal_rows, zonal, preferred_element_type=jnp.float32).astype(
        jnp.bfloat16
    )
    pert_fields = perturbs.reshape(mem_dev, levels, lat_rows, lon_cols)
    weight = static_weight[:, None, None]
    filtered = lax.all_to_all(grid, "lon", split_axis=2, concat_axis=0, tiled=True).reshape(
        mem_dev + 1, levels, lat_rows, lon_cols
    )
    ensemble = jnp.einsum(
        "mlxn,mlxn->lxn", pert_fields, filtered[:mem_dev], preferred_element_type=jnp.float32
    )
    static_part = filtered[mem_dev].astype(jnp.float32)
    own = first_mem * weight * static_part + (1.0 - weight) * ensemble
    total = lax.psum(own, "mem")
    return total.reshape(levels, 1, 1, cell_count)


LANES = 128
GROUP = 8


def split_members_kernel(cells_ref, extra_ref, *refs, rows, cols, members):
    out_ref, scratch = refs[-2:]
    tiles = cols // LANES
    for y in range(rows):
        for t in range(tiles):
            at = y * cols + t * LANES
            scratch[t, y * GROUP : (y + 1) * GROUP, :] = cells_ref[
                0, :, at : at + LANES
            ].astype(jnp.float32)
    for m in range(GROUP):
        for t in range(tiles):
            out_ref[0, m, :, t * LANES : (t + 1) * LANES] = scratch[
                t, pl.ds(m, rows, stride=GROUP), :
            ].astype(jnp.bfloat16)

    @pl.when(pl.program_id(0) == members // GROUP)
    def _():
        out_ref[0, members % GROUP] = extra_ref[0]


def split_members(cells, extra, level, lat_rows, lon_cols, after=()):
    members = cells.shape[1]
    groups = -(-(members + 1) // GROUP)
    rows = lat_rows // 4
    return pl.pallas_call(
        functools.partial(
            split_members_kernel, rows=rows, cols=lon_cols, members=members
        ),
        grid=(groups, lat_rows // rows),
        in_specs=[
            pl.BlockSpec((1, GROUP, rows * lon_cols), lambda g, y: (level, g, y)),
            pl.BlockSpec((1, rows, lon_cols), lambda g, y: (level, y, 0)),
        ]
        + [pl.BlockSpec(memory_space=pl.ANY)] * len(after),
        out_specs=pl.BlockSpec((1, GROUP, rows, lon_cols), lambda g, y: (g, 0, y, 0)),
        out_shape=jax.ShapeDtypeStruct((groups, GROUP, lat_rows, lon_cols), jnp.bfloat16),
        scratch_shapes=[pltpu.VMEM((lon_cols // LANES, rows * GROUP, LANES), jnp.float32)],
        name="split_members",
    )(cells, extra, *after)


def to_waves_kernel(place_ref, strips_ref, zonal_ref, *refs, parts):
    out_refs = refs[-parts:]
    count, per, rows, cols = strips_ref.shape
    waves = zonal_ref.shape[2]
    total = jnp.zeros((per * rows, waves), jnp.float32)
    for s in range(count):
        total += jnp.dot(
            strips_ref[s].reshape(per * rows, cols),
            zonal_ref[s],
            preferred_element_type=jnp.float32,
        )
    result = total.astype(jnp.bfloat16).reshape(per, rows, waves)
    for r, out_ref in enumerate(out_refs):

        @pl.when(pl.program_id(0) == r)
        def _():
            out_ref[...] = result


def to_waves(place, strips, zonal, parts, after=()):
    count, fields, rows, cols = strips.shape
    waves = zonal.shape[2]
    per = fields // parts
    return pl.pallas_call(
        functools.partial(to_waves_kernel, parts=parts),
        grid_spec=pltpu.PrefetchScalarGridSpec(
            num_scalar_prefetch=1,
            grid=(parts,),
            in_specs=[
                pl.BlockSpec(
                    (count, per, rows, cols), lambda r, at: (0, (at[0] + r) % parts, 0, 0)
                ),
                pl.BlockSpec((count, cols, waves), lambda r, at: (0, 0, 0)),
            ]
            + [pl.BlockSpec(memory_space=pl.ANY)] * len(after),
            out_specs=[pl.BlockSpec((per, rows, waves), lambda r, at: (0, 0, 0))] * parts,
        ),
        out_shape=[jax.ShapeDtypeStruct((per, rows, waves), jnp.bfloat16)] * parts,
        name="to_waves",
    )(place, strips, zonal, *after)


def meridional_kernel(place_ref, which_ref, *refs, parts):
    ins, (spectrum_ref, basis_ref, basis_t_ref) = refs[:parts], refs[parts : parts + 3]
    outs, field_ref = refs[-parts - 1 : -1], refs[-1]
    _, rows, waves = ins[0].shape
    place = place_ref[0]
    for r in range(parts):
        source = (place + parts - r) % parts
        field_ref[pl.ds(pl.multiple_of(source * rows, 64), rows), :] = ins[r][0]
    coef = jnp.dot(basis_t_ref[...], field_ref[...], preferred_element_type=jnp.float32)
    scaled = (coef * spectrum_ref[0]).astype(jnp.bfloat16)
    back = jnp.dot(basis_ref[...], scaled, preferred_element_type=jnp.float32)
    field_ref[...] = back.astype(jnp.bfloat16)
    for r in range(parts):
        target = (place + r) % parts
        outs[r][0] = field_ref[pl.ds(pl.multiple_of(target * rows, 64), rows), :]


def meridional(place, which, bands, spectra, basis, basis_t, after=()):
    parts = len(bands)
    fields, rows, waves = bands[0].shape
    kept = basis.shape[1]
    band = pl.BlockSpec((1, rows, waves), lambda f, at, w: (f, 0, 0))
    return pl.pallas_call(
        functools.partial(meridional_kernel, parts=parts),
        grid_spec=pltpu.PrefetchScalarGridSpec(
            num_scalar_prefetch=2,
            grid=(fields,),
            in_specs=[band] * parts
            + [
                pl.BlockSpec((1, kept, waves), lambda f, at, w: (w[f], 0, 0)),
                pl.BlockSpec(basis.shape, lambda f, at, w: (0, 0)),
                pl.BlockSpec(basis_t.shape, lambda f, at, w: (0, 0)),
            ]
            + [pl.BlockSpec(memory_space=pl.ANY)] * len(after),
            out_specs=[band] * parts,
            scratch_shapes=[pltpu.VMEM((parts * rows, waves), jnp.bfloat16)],
        ),
        out_shape=[jax.ShapeDtypeStruct((fields, rows, waves), jnp.bfloat16)] * parts,
        name="meridional",
    )(place, which, *bands, spectra, basis, basis_t, *after)


def to_grid_kernel(place_ref, *refs, parts):
    ins, zonal_t_ref, out_ref = refs[:parts], refs[parts], refs[-1]
    per, rows, waves = ins[0].shape
    count, _, cols = zonal_t_ref.shape
    for r in range(parts):

        @pl.when(pl.program_id(0) == r)
        def _():
            field = ins[r][...].reshape(per * rows, waves)
            for s in range(count):
                strip = jnp.dot(field, zonal_t_ref[s], preferred_element_type=jnp.float32)
                out_ref[s] = strip.astype(jnp.bfloat16).reshape(per, rows, cols)


def to_grid(place, bands, zonal_t, after=()):
    parts = len(bands)
    per, rows, waves = bands[0].shape
    count, _, cols = zonal_t.shape
    return pl.pallas_call(
        functools.partial(to_grid_kernel, parts=parts),
        grid_spec=pltpu.PrefetchScalarGridSpec(
            num_scalar_prefetch=1,
            grid=(parts,),
            in_specs=[pl.BlockSpec((per, rows, waves), lambda r, at: (0, 0, 0))] * parts
            + [pl.BlockSpec(zonal_t.shape, lambda r, at: (0, 0, 0))]
            + [pl.BlockSpec(memory_space=pl.ANY)] * len(after),
            out_specs=pl.BlockSpec(
                (count, per, rows, cols), lambda r, at: (0, (at[0] + parts - r) % parts, 0, 0)
            ),
        ),
        out_shape=jax.ShapeDtypeStruct((count, per * parts, rows, cols), jnp.bfloat16),
        name="to_grid",
    )(place, *bands, zonal_t, *after)


def combine_kernel(scale_ref, pert_ref, grid_ref, out_ref, *, members):
    total = jnp.zeros(out_ref.shape, jnp.float32)
    for m in range(members):
        g, i = divmod(m, GROUP)
        total += pert_ref[g, i].astype(jnp.float32) * grid_ref[g, i].astype(jnp.float32)
    g, i = divmod(members, GROUP)
    static = grid_ref[g, i].astype(jnp.float32)
    out_ref[...] = scale_ref[0] * static + scale_ref[1] * total


def combine(scales, perts, grids, members):
    groups, per, rows, cols = grids.shape
    block = rows // 6
    return pl.pallas_call(
        functools.partial(combine_kernel, members=members),
        grid=(rows // block,),
        in_specs=[
            pl.BlockSpec(memory_space=pltpu.SMEM),
            pl.BlockSpec((groups, per, block, cols), lambda y: (0, 0, y, 0)),
            pl.BlockSpec((groups, per, block, cols), lambda y: (0, 0, y, 0)),
        ],
        out_specs=pl.BlockSpec((block, cols), lambda y: (y, 0)),
        out_shape=jax.ShapeDtypeStruct((rows, cols), jnp.float32),
        name="combine",
    )(scales, perts, grids)


def shards_by_field(
    control, perturbs, static_input, lat_basis, local_spectrum, static_spectrum, static_weight
):
    members, levels = control.shape[:2]
    cell_count = control.shape[-1]
    n_lat, n_lon, n_mem = lax.axis_size("lat"), lax.axis_size("lon"), lax.axis_size("mem")
    lat_rows = NLAT // n_lat
    lon_cols = cell_count // lat_rows
    cells = control.transpose(1, 0, 2, 3, 4).reshape(levels, members, cell_count)
    pert_cells = perturbs.transpose(1, 0, 2, 3, 4).reshape(levels, members, cell_count)
    static_fields = static_input.reshape(levels, lat_rows, lon_cols)

    lat_at = lax.axis_index("lat").astype(jnp.int32)
    place = lat_at.reshape(1)

    def exchange(x, axis):
        return lax.all_to_all(x, axis, split_axis=0, concat_axis=0, tiled=True)

    def shift(parts):
        return [
            lax.ppermute(x, "lat", [(i, (i + r) % n_lat) for i in range(n_lat)]) if r else x
            for r, x in enumerate(parts)
        ]

    own_spectra = jnp.stack([local_spectrum.T, static_spectrum.T])
    spectra = jnp.zeros((n_lat,) + own_spectra.shape, jnp.float32)
    spectrum_parts = shift([own_spectra] * n_lat)
    for r, x in enumerate(spectrum_parts):
        spectra = lax.dynamic_update_slice_in_dim(spectra, x[None], (lat_at - r) % n_lat, 0)
    spectra = spectra.transpose(1, 3, 0, 2).reshape(2, lat_basis.shape[1], KLON)
    zonal = lax.optimization_barrier(zonal_table())
    zonal_t = zonal.reshape(n_lon, lon_cols, KLON).transpose(0, 2, 1)
    zonal = zonal.reshape(n_lon, lon_cols, KLON)
    basis_t = lat_basis.T
    perts = [split_members(pert_cells, static_fields, l, lat_rows, lon_cols) for l in range(levels)]

    first = lax.axis_index("lon") * GROUP + lat_at * (GROUP // n_lat)
    slot = first + jnp.arange(GROUP // n_lat, dtype=jnp.int32)
    which = (slot >= members).astype(jnp.int32)
    first_mem = (lax.axis_index("mem") == 0).astype(jnp.float32)

    strips, waves, bands, scaled, grids = [], [], [], [], []

    def start(level, after):
        f = split_members(cells, static_fields, level, lat_rows, lon_cols, after)
        strips.append(exchange(f, "lon"))

    def forward(level, after):
        waves.append(to_waves(place, strips[level], zonal, n_lat, after))
        bands.append(shift(waves[level]))

    def middle(level, after):
        scaled.append(
            meridional(place, which, bands[level], spectra, lat_basis, basis_t, after)
        )

    def back(level, after):
        grids.append(to_grid(place, shift(scaled[level]), zonal_t, after))

    last, near = levels - 1, 1 % n_lat
    start(0, ())
    if levels > 1:
        start(1, (zonal, spectra))
    for level in range(levels):
        forward(level, ())
        if level + 2 < levels:
            start(level + 2, tuple(bands[level][1:]))
    for level in range(levels):
        after = (bands[level + 1][near],) if level < last else ()
        if 0 < level < last:
            back(level - 1, (waves[level + 1][0],))
            after += (grids[level - 1],)
        middle(level, after)
    if levels > 1:
        back(last - 1, (scaled[last][0],))
    back(last, ())
    grids = [exchange(g, "lon") for g in grids]
    results = []
    for level in range(levels):
        weight = static_weight[level]
        scales = jnp.stack([first_mem * weight, 1.0 - weight])
        own = combine(scales, perts[level], grids[level], members)
        other = lax.ppermute(own, "mem", [(i, (i + 1) % n_mem) for i in range(n_mem)])
        results.append(own + other)
    return jnp.stack(results).reshape(levels, 1, 1, cell_count)


def shards(
    control, perturbs, static_input, lat_basis, local_spectrum, static_spectrum, static_weight
):
    members = control.shape[0]
    n_lat, n_lon, n_mem = lax.axis_size("lat"), lax.axis_size("lon"), lax.axis_size("mem")
    lat_rows = NLAT // n_lat
    lon_cols = control.shape[-1] // lat_rows
    by_field = (
        members + 1 == n_lon * GROUP
        and GROUP % n_lat == 0
        and n_mem == 2
        and lon_cols % LANES == 0
        and lat_rows % 64 == 0
    )
    run = shards_by_field if by_field else shards_general
    return run(
        control, perturbs, static_input, lat_basis, local_spectrum, static_spectrum, static_weight
    )


def solution(mesh):
    return jax.shard_map(
        shards,
        mesh=mesh,
        in_specs=(
            P("mem", None, "lat", "lon", None),
            P("mem", None, "lat", "lon", None),
            P(None, "lat", "lon", None),
            P(),
            P(None, "lat"),
            P(None, "lat"),
            P(),
        ),
        out_specs=P(None, "lat", "lon", None),
        check_vma=False,
    )
```
